32 devices in a mesh: blk: 16 (over z, y, core), col: 2 (over x).
Axes of the slice: x: 2, y: 2, z: 4, core: 2. Of those that a mesh axis runs over, the one named last changes fastest.
Arguments:
- counts: float32 [8192, 8192], P('blk', 'col'), may hold values from 0.1 to 10
- merge_map: int32 [8192, 1], replicated, may hold values from 0 to 4095, as said below
Outputs:
- merged: float32 [4096, 4096], P('blk', 'col')
- block_terms: float32 [4096], P('blk')
The draws below stay inside these ranges and needn't reach their ends.
Inputs may be any that keep to these rules, and one draw needn't show every extreme that they name: `merge_map`: every new block is the image of exactly two old blocks. Let the owner of new block r be r // 256. The 512 old blocks i with i // 512 = s, for each s, map to new blocks of exactly 8 distinct owners, exactly 64 old blocks to each of them, and each owner receives from exactly 8 such s.
All inputs are finite; a program needn't handle non-finite values.
Results may differ from the reference program's by a relative error of at most 0.0003.
Values sent between devices are 32-bit elements; how exact they have to be, the bound alone decides.
No kernel may reach another device: no remote copies, remote signals or barrier semaphores. Data moves between devices by JAX's collectives and lax.ppermute only.
A program may use at most 128 MiB of HBM per device.

```python
import math
import jax
import jax.numpy as jnp

B = 8192
NB = 4096
ROWS_DEV = 512
OWNED_DEV = 256
FANOUT = 8
SLOT_CAP = 64
N_BLK = 16


def draw_merge_map(key, part):
    base = jax.random.fold_in(key, 11)
    key_src, key_off, key_row, key_slot = jax.random.split(base, 4)
    placing = jax.random.permutation(key_src, N_BLK)
    offsets = jax.random.permutation(key_off, N_BLK)[:FANOUT]
    row_keys = jax.random.split(key_row, N_BLK)
    ranking = jax.vmap(lambda single: jax.random.permutation(single, ROWS_DEV))(row_keys)
    group = ranking // SLOT_CAP
    within = ranking % SLOT_CAP
    owner = (placing[:, None] + offsets[group]) % N_BLK
    slot_keys = jax.random.split(key_slot, N_BLK)
    shuffles = jax.vmap(lambda single: jax.random.permutation(single, ROWS_DEV))(slot_keys)
    placed = shuffles[owner, group * SLOT_CAP + within]
    new_ids = owner * OWNED_DEV + placed // 2
    return new_ids.reshape(B, 1).astype(jnp.int32)


def block_scale(key, shape, shards, low, largest):
    def one(dim, blocks):
        heights = jax.random.uniform(jax.random.fold_in(jax.random.fold_in(key, 6), dim), (blocks,), jnp.float32, low / len(shards), largest / len(shards))
        return jnp.repeat(jnp.exp(heights), shape[dim] // blocks).reshape((-1,) + (1,) * (len(shape) - dim - 1))

    factor_of = one(*shards[0])
    for cut in shards[1:]:
        factor_of = factor_of * one(*cut)
    return factor_of


def setup_inputs(seed: int = 0) -> dict:
    splits = jax.random.split(jax.random.key(seed), 3)
    counts = jnp.clip(jnp.exp(math.log(10.0) - 4.6051702 * jax.random.uniform(splits[0], (B, B), jnp.float32) ** block_scale(splits[0], (B, B), ((0, 16), (1, 2)), -0.2, 0.2)), 0.1, 10.0)
    merge_map = draw_merge_map(jax.random.fold_in(splits[2], 71), 0)
    return {"counts": counts, "merge_map": merge_map}


def reference(counts, merge_map):
    ids = merge_map[:, 0].astype(jnp.int32)
    rows = jax.ops.segment_sum(counts, ids, num_segments=NB)
    merged = jax.ops.segment_sum(rows.T, ids, num_segments=NB).T
    out_total = jnp.sum(merged, axis=1)
    in_total = jnp.sum(merged, axis=0)
    total = jnp.sum(in_total)
    share = merged / out_total[:, None]
    ratio = merged * total / (out_total[:, None] * in_total[None, :])
    block_terms = jnp.sum(share * jnp.log(ratio), axis=1)
    return merged, block_terms
```

```python
import functools

import jax
import jax.numpy as jnp
from jax import lax
from jax.experimental import pallas as pl
from jax.experimental.pallas import tpu as pltpu
from jax.sharding import PartitionSpec as P

PARTS = (2, 4, 4, 4, 2)
F32, BF16, I32 = jnp.float32, jnp.bfloat16, jnp.int32


def widths(owned_cols):
    unit = owned_cols // sum(PARTS)
    return [p * unit for p in PARTS] if unit % 128 == 0 else [owned_cols]


def split(x):
    hi = x.astype(BF16)
    return hi, (x - hi.astype(F32)).astype(BF16)


def hot(labels, count, base=0):
    index = lax.broadcasted_iota(I32, (count, labels.shape[1]), 0) + base
    return jnp.where(index == labels, 1.0, 0.0).astype(BF16)


def mxu(a, b, dims):
    return lax.dot_general(a, b, (dims, ((), ())), preferred_element_type=F32)


def call(kernel, flops, nbytes, **kw):
    return pl.pallas_call(
        kernel, cost_estimate=pl.CostEstimate(flops=flops, bytes_accessed=nbytes, transcendentals=0), **kw
    )


def columns_kernel(start, owned, present_ref, pos_ref, counts_ref, *out_refs):
    rows, width = out_refs[0].shape
    k = pl.program_id(0)
    per_column = present_ref.shape[1] // len(out_refs)

    @pl.when(k == 0)
    def _():
        for out_ref in out_refs:
            out_ref[...] = jnp.zeros_like(out_ref)

    hi, lo = split(counts_ref[...])
    both = jnp.concatenate([hi, lo], axis=0)
    for c, out_ref in enumerate(out_refs):
        for b in range(width // owned):
            block = c * per_column + start // owned + b

            @pl.when(present_ref[k, block] > 0)
            def _():
                part = mxu(both, hot(pos_ref[...], owned, block * owned), ((1,), (1,)))
                out_ref[:, b * owned : (b + 1) * owned] += part[:rows] + part[rows:]


def merge_columns(counts, pos, present, owned, columns, start, width):
    rows, cols = counts.shape
    tile = cols // present.shape[0]
    return call(
        functools.partial(columns_kernel, start, owned),
        2 * rows * cols * columns * width, 4 * rows * (cols + columns * width),
        grid_spec=pltpu.PrefetchScalarGridSpec(
            num_scalar_prefetch=1,
            grid=(cols // tile,),
            in_specs=[pl.BlockSpec((1, tile), lambda k, _: (0, k)), pl.BlockSpec((rows, tile), lambda k, _: (0, k))],
            out_specs=[pl.BlockSpec((rows, width), lambda k, _: (0, 0))] * columns,
        ),
        out_shape=[jax.ShapeDtypeStruct((rows, width), F32)] * columns,
    )(present, pos, counts)


def slots_kernel(pos_ref, *refs):
    ins, out_ref, sum_ref, table = refs[:-3], refs[-3], refs[-2], refs[-1]

    @pl.when(pl.program_id(0) == 0)
    def _():
        table[...] = hot(pos_ref[...], table.shape[0])

    total = ins[0][...]
    for ref in ins[1:]:
        total += ref[...]
    sum_ref[...] = jnp.sum(total, axis=0, keepdims=True)
    hi, lo = split(total)
    out_ref[...] = mxu(table[...], hi, ((1,), (0,))) + mxu(table[...], lo, ((1,), (0,)))


def fill_slots(pos, ins, slots):
    rows, width = ins[0].shape
    tile = min(width, 256)
    return call(
        slots_kernel, 4 * slots * rows * width, 4 * width * (rows * len(ins) + slots),
        grid=(width // tile,),
        in_specs=[pl.BlockSpec((1, rows), lambda k: (0, 0))] + [pl.BlockSpec((rows, tile), lambda k: (0, k))] * len(ins),
        out_specs=[pl.BlockSpec((slots, tile), lambda k: (0, k)), pl.BlockSpec((1, tile), lambda k: (0, k))],
        out_shape=[jax.ShapeDtypeStruct((slots, width), F32), jax.ShapeDtypeStruct((1, width), F32)],
        scratch_shapes=[pltpu.VMEM((slots, rows), BF16)],
    )(pos, *ins)


def rows_kernel(pos_ref, got_ref, keep_ref, send_ref):
    peers, _, cap, tile = got_ref.shape
    for side, ref in enumerate((keep_ref, send_ref)):
        hi, lo = split(got_ref[:, side].reshape(peers * cap, tile))
        table = hot(pos_ref[side : side + 1, :], ref.shape[0])
        ref[...] = mxu(table, hi, ((1,), (0,))) + mxu(table, lo, ((1,), (0,)))


def merge_rows(pos, got, owned):
    peers, _, cap, width = got.shape
    tile = min(width, 256)
    return call(
        rows_kernel, 8 * owned * peers * cap * width, 4 * width * (2 * owned + 2 * peers * cap),
        grid=(width // tile,),
        in_specs=[
            pl.BlockSpec((2, peers * cap), lambda k: (0, 0)),
            pl.BlockSpec((peers, 2, cap, tile), lambda k: (0, 0, 0, k)),
        ],
        out_specs=[pl.BlockSpec((owned, tile), lambda k: (0, k))] * 2,
        out_shape=[jax.ShapeDtypeStruct((owned, width), F32)] * 2,
    )(pos, got)


def fold(x):
    return sum(x[:, j : j + 128] for j in range(0, x.shape[1], 128))


def terms(block, in_total, new):
    return fold(block * jnp.log(block * (new / in_total))), fold(block)


def early_kernel(plan, new, in_total_ref, *refs):
    n = len(plan)
    keeps, others, (merged_ref, logs_ref, out_ref) = refs[:n], refs[n : 2 * n], refs[2 * n :]
    start, logs, out = 0, 0.0, 0.0
    for keep, other, width in zip(keeps, others, plan):
        block = keep[...] + other[...]
        merged_ref[:, start : start + width] = block
        more = terms(block, in_total_ref[:, start : start + width], new)
        logs, out, start = logs + more[0], out + more[1], start + width
    logs_ref[...], out_ref[...] = logs, out


def finish_early(plan, new, in_total, keeps, others):
    owned, total = keeps[0].shape[0], sum(plan)
    n, done = len(plan) - 1, sum(plan[:-1])
    tile = min(owned, 64)
    blocks = [pl.BlockSpec((tile, w), lambda k: (k, 0)) for w in plan[:-1]]
    lanes = pl.BlockSpec((tile, 128), lambda k: (k, 0))
    return call(
        functools.partial(early_kernel, plan[:-1], new), 20 * owned * done, 12 * owned * done,
        grid=(owned // tile,),
        in_specs=[pl.BlockSpec((1, total), lambda k: (0, 0))] + blocks * 2,
        out_specs=[pl.BlockSpec((tile, done), lambda k: (k, 0)), lanes, lanes],
        out_shape=[jax.ShapeDtypeStruct((owned, total), F32)] + [jax.ShapeDtypeStruct((owned, 128), F32)] * 2,
    )(in_total, *keeps[:n], *others[:n])


def last_kernel(new, in_total_ref, keep_ref, other_ref, *refs):
    merged_ref, part_ref = refs[-2:]
    width = keep_ref.shape[1]
    block = keep_ref[...] + other_ref[...]
    merged_ref[...] = block
    logs, out = terms(block, in_total_ref[:, in_total_ref.shape[1] - width :], new)
    if len(refs) > 2:
        logs, out = logs + refs[1][...], out + refs[2][...]
    row = lax.broadcasted_iota(I32, part_ref.shape, 0)
    logs = jnp.sum(logs.T, axis=0, keepdims=True)
    out = jnp.sum(out.T, axis=0, keepdims=True)
    total = jnp.sum(in_total_ref[...], axis=1, keepdims=True)
    part_ref[...] = jnp.where(row == 0, logs, jnp.where(row == 1, out, total))


def finish_last(plan, new, in_total, keep, other, early):
    owned, width, total = keep.shape[0], plan[-1], sum(plan)
    at = (total - width) // width
    whole = pl.BlockSpec((owned, width), lambda k: (0, 0))
    lanes = [pl.BlockSpec((owned, 128), lambda k: (0, 0))] * 2
    return call(
        functools.partial(last_kernel, new), 20 * owned * width, 12 * owned * width,
        grid=(1,),
        in_specs=[pl.BlockSpec((1, total), lambda k: (0, 0)), whole, whole]
        + ([pl.BlockSpec(memory_space=pl.ANY)] + lanes if early else []),
        out_specs=[pl.BlockSpec((owned, width), lambda k: (0, at)), pl.BlockSpec((8, owned), lambda k: (0, 0))],
        out_shape=[jax.ShapeDtypeStruct((owned, total), F32), jax.ShapeDtypeStruct((8, owned), F32)],
        input_output_aliases={3: 0} if early else {},
    )(in_total, keep, other, *early)


def tags_of(ids, mine, capacity):
    rank = jnp.cumsum(mine.astype(I32), axis=1) - 1
    hit = mine[:, None, :] & (rank[:, None, :] == jnp.arange(capacity, dtype=I32)[None, :, None])
    return jnp.max(jnp.where(hit, ids[:, None, :], -1), axis=2)


def body(counts, merge_map):
    rows, cols = counts.shape
    groups, columns = lax.axis_size("blk"), lax.axis_size("col")
    blk, col = lax.axis_index("blk"), lax.axis_index("col")
    ids = merge_map[:, 0]
    new = ids.shape[0] // 2
    owned, owned_cols = new // groups, new // columns
    fanout = min(groups // 2, rows // 2)
    cap = rows // fanout
    half = groups // 2
    plan = widths(owned_cols)
    starts = [sum(plan[:q]) for q in range(len(plan))]
    row_labels = lax.dynamic_slice_in_dim(ids, blk * rows, rows, 0)
    col_labels = lax.dynamic_slice_in_dim(ids, col * cols, cols, 0)

    step_of = lax.rem(col_labels // owned_cols - col + columns, columns)
    col_pos = step_of * owned_cols + lax.rem(col_labels, owned_cols)
    mapped = (col_pos // owned).reshape(cols // rows, rows, 1) == jnp.arange(groups, dtype=I32)
    present = jnp.max(mapped.astype(I32), axis=1)

    owner = row_labels // owned
    table = (owner[:, None] == jnp.arange(groups, dtype=I32)[None, :]).astype(I32)
    rank = jnp.sum(jnp.cumsum(table, axis=0) * table, axis=1) - 1
    place = lax.rem(owner, half) * 2 + (owner // half != blk // half).astype(I32)
    row_pos = (place * cap + rank)[None, :]

    base = (blk // half) * half
    peers = lax.dynamic_slice_in_dim(ids.reshape(groups, rows), base, half, 0)
    take_pos = []
    for agg in (blk, lax.rem(blk + half, groups)):
        tags = tags_of(peers, peers // owned == agg, cap).reshape(-1)
        take_pos.append(jnp.where(tags < 0, -1, tags - agg * owned))
    take_pos = jnp.stack(take_pos)

    sums, keeps, others = [], [], []
    for q, width in enumerate(plan):
        parts = list(merge_columns(counts, col_pos[None, :], present, owned, columns, starts[q], width))
        for step in range(1, columns):
            parts[step] = lax.ppermute(parts[step], "col", [(i, (i + step) % columns) for i in range(columns)])
        slotted, column_sum = fill_slots(row_pos, parts, groups * cap)
        sums.append(column_sum)
        got = lax.all_to_all(
            slotted.reshape(half, 2, cap, width), "blk", split_axis=0, concat_axis=0, tiled=True,
            axis_index_groups=[list(range(half)), list(range(half, groups))],
        )
        keep, send = merge_rows(take_pos, got, owned)
        others.append(lax.ppermute(send, "blk", [(i, (i + half) % groups) for i in range(groups)]))
        keeps.append(keep)
    sums = jnp.broadcast_to(jnp.concatenate(sums, axis=1), (groups, owned_cols))
    sums = lax.all_to_all(sums, "blk", split_axis=0, concat_axis=0, tiled=True)
    in_total = jnp.sum(sums, axis=0, keepdims=True)
    early = ()
    if len(plan) > 1:
        early = finish_early(plan, new, in_total, keeps, others)
    merged, part = finish_last(plan, new, in_total, keeps[-1], others[-1], early)
    if columns == 2:
        part += lax.ppermute(part, "col", [(0, 1), (1, 0)])
    else:
        part = lax.psum(part, "col")
    block_terms = part[0] / part[1] + jnp.log(part[2] / (part[1] * new))
    return (merged, block_terms)


def solution(mesh):
    placed = (P("blk", "col"), P())
    return jax.shard_map(body, mesh=mesh, in_specs=placed, out_specs=(P("blk", "col"), P("blk")), check_vma=False)
```

```python
import functools

import jax
import jax.numpy as jnp
from jax import lax
from jax.experimental import pallas as pl
from jax.experimental.pallas import tpu as pltpu
from jax.sharding import PartitionSpec as P

PARTS = (2, 4, 4, 4, 2)
VMEM = 24 * 2**20
F32, BF16, I32 = jnp.float32, jnp.bfloat16, jnp.int32


def widths(owned_cols):
    unit = owned_cols // sum(PARTS)
    return [p * unit for p in PARTS] if unit % 128 == 0 else [owned_cols]


def split(x):
    hi = x.astype(BF16)
    return hi, (x - hi.astype(F32)).astype(BF16)


def hot(labels, count, base=0):
    index = lax.broadcasted_iota(I32, (count, labels.shape[1]), 0) + base
    return jnp.where(index == labels, 1.0, 0.0).astype(BF16)


def mxu(a, b, dims):
    return lax.dot_general(a, b, (dims, ((), ())), preferred_element_type=F32)


def call(kernel, flops, nbytes, **kw):
    return pl.pallas_call(
        kernel,
        cost_estimate=pl.CostEstimate(flops=flops, bytes_accessed=nbytes, transcendentals=0),
        compiler_params=pltpu.CompilerParams(vmem_limit_bytes=VMEM),
        **kw,
    )


def columns_kernel(start, owned, first, present_ref, pos_ref, x_ref, *refs):
    sources = present_ref.shape[0]
    tile = x_ref.shape[1] // sources
    halves_ref, out_refs = (refs[0], refs[1:]) if first else (x_ref, refs)
    rows, width = out_refs[0].shape
    per_column = present_ref.shape[1] // len(out_refs)
    for out_ref in out_refs:
        out_ref[...] = jnp.zeros_like(out_ref)

    def step(k, carry):
        at = pl.ds(pl.multiple_of(k * tile, tile), tile)
        if first:
            halves_ref[:rows, at], halves_ref[rows:, at] = split(x_ref[:, at])
        for c, out_ref in enumerate(out_refs):
            for b in range(width // owned):
                block = c * per_column + start // owned + b

                @pl.when(present_ref[k, block] > 0)
                def _():
                    part = mxu(halves_ref[:, at], hot(pos_ref[:, at], owned, block * owned), ((1,), (1,)))
                    out_ref[:, b * owned : (b + 1) * owned] += part[:rows] + part[rows:]

        return carry

    lax.fori_loop(0, sources, step, 0)


def merge_columns(x, pos, present, owned, columns, start, width, first):
    rows, cols = x.shape if first else (x.shape[0] // 2, x.shape[1])
    vmem = pl.BlockSpec(memory_space=pltpu.VMEM)
    halves = [jax.ShapeDtypeStruct((2 * rows, cols), BF16)] if first else []
    return call(
        functools.partial(columns_kernel, start, owned, first),
        2 * rows * cols * columns * width, 4 * rows * (cols + columns * width),
        in_specs=[pl.BlockSpec(memory_space=pltpu.SMEM), vmem, vmem],
        out_specs=[vmem] * (len(halves) + columns),
        out_shape=halves + [jax.ShapeDtypeStruct((rows, width), F32)] * columns,
    )(present, pos, x)


def slots_kernel(carrier, pos_ref, *refs):
    ins, out_ref, sum_ref, table = refs[:-3], refs[-3], refs[-2], refs[-1]
    known_ref, ins = (ins[0], ins[1:]) if carrier is not None else (None, ins)
    peers, depth, tile = out_ref.shape
    used = table.shape[0] // peers

    @pl.when(pl.program_id(0) == 0)
    def _():
        table[...] = hot(pos_ref[...], table.shape[0])

    total = ins[0][...]
    for ref in ins[1:]:
        total += ref[...]
    column_sum = jnp.sum(total, axis=0, keepdims=True)
    sum_ref[...] = column_sum
    hi, lo = split(total)
    filled = mxu(table[...], hi, ((1,), (0,))) + mxu(table[...], lo, ((1,), (0,)))
    out_ref[:, :used] = filled.reshape(peers, used, tile)
    if carrier is not None:
        row = lax.broadcasted_iota(I32, known_ref.shape, 0)
        sums = jnp.where(row == carrier, column_sum, known_ref[...])
        out_ref[:, used:] = jnp.broadcast_to(sums[None], (peers, depth - used, tile))


def fill_slots(pos, ins, peers, slots, carrier=None, known=None):
    rows, width = ins[0].shape
    tile = min(width, 256)
    depth = slots // peers + (0 if carrier is None else 8)
    extra = [] if carrier is None else [known]
    return call(
        functools.partial(slots_kernel, carrier),
        4 * slots * rows * width, 4 * width * (rows * len(ins) + slots),
        grid=(width // tile,),
        in_specs=[pl.BlockSpec((1, rows), lambda k: (0, 0))]
        + [pl.BlockSpec((8, tile), lambda k: (0, k))] * len(extra)
        + [pl.BlockSpec((rows, tile), lambda k: (0, k))] * len(ins),
        out_specs=[pl.BlockSpec((peers, depth, tile), lambda k: (0, 0, k)), pl.BlockSpec((1, tile), lambda k: (0, k))],
        out_shape=[jax.ShapeDtypeStruct((peers, depth, width), F32), jax.ShapeDtypeStruct((1, width), F32)],
        scratch_shapes=[pltpu.VMEM((slots, rows), BF16)],
    )(pos, *extra, *ins)


def rows_kernel(pos_ref, got_ref, keep_ref, send_ref, *sum_refs):
    peers, _, tile = got_ref.shape
    owned, cap = keep_ref.shape[0], pos_ref.shape[1] // peers
    for side, ref in enumerate((keep_ref, send_ref)):
        hi, lo = split(got_ref[:, side * cap : (side + 1) * cap].reshape(peers * cap, tile))
        table = hot(pos_ref[side : side + 1, :], owned)
        ref[:owned] = mxu(table, hi, ((1,), (0,))) + mxu(table, lo, ((1,), (0,)))
    for ref in sum_refs:
        ref[...] = jnp.sum(got_ref[:, 2 * cap :], axis=0)
        send_ref[owned:] = ref[...]


def merge_rows(pos, got, owned, carrier):
    peers, depth, width = got.shape
    slots = pos.shape[1]
    tile = min(width, 256)
    heights = [owned, owned + 8, 8] if carrier else [owned, owned]
    return call(
        rows_kernel, 8 * owned * slots * width, 4 * width * (2 * owned + 2 * slots),
        grid=(width // tile,),
        in_specs=[pl.BlockSpec((2, slots), lambda k: (0, 0)), pl.BlockSpec((peers, depth, tile), lambda k: (0, 0, k))],
        out_specs=[pl.BlockSpec((h, tile), lambda k: (0, k)) for h in heights],
        out_shape=[jax.ShapeDtypeStruct((h, width), F32) for h in heights],
    )(pos, got)


def fold(x):
    return sum(x[:, j : j + 128] for j in range(0, x.shape[1], 128))


def terms(block, in_total, new):
    return fold(block * jnp.log(block * (new / in_total))), fold(block)


def early_kernel(plan, new, in_total_ref, *refs):
    ins, (merged_ref, logs_ref, out_ref) = list(refs[:-3]), refs[-3:]
    start, logs, out = 0, 0.0, 0.0
    for q, (width, parts) in enumerate(plan):
        block = sum(ins.pop(0)[...] for _ in range(parts))
        merged_ref[:, start : start + width] = block
        more = terms(block, in_total_ref[q : q + 1, :width], new)
        logs, out, start = logs + more[0], out + more[1], start + width
    logs_ref[...], out_ref[...] = logs, out


def finish_early(plan, new, in_total, chunks):
    owned, total, done = chunks[0][0].shape[0], sum(plan), sum(plan[:-1])
    tile = min(owned, 64)
    lanes = pl.BlockSpec((tile, 128), lambda k: (k, 0))
    return call(
        functools.partial(early_kernel, [(w, len(c)) for w, c in zip(plan, chunks)], new),
        20 * owned * done, 12 * owned * done,
        grid=(owned // tile,),
        in_specs=[pl.BlockSpec(in_total.shape, lambda k: (0, 0))]
        + [pl.BlockSpec((tile, w), lambda k: (k, 0)) for w, c in zip(plan, chunks) for _ in c],
        out_specs=[pl.BlockSpec((tile, done), lambda k: (k, 0)), lanes, lanes],
        out_shape=[jax.ShapeDtypeStruct((owned, total), F32)] + [jax.ShapeDtypeStruct((owned, 128), F32)] * 2,
    )(in_total, *(x for c in chunks for x in c))


def last_kernel(chunk, new, in_total_ref, keep_ref, other_ref, *refs):
    merged_ref, part_ref = refs[-2:]
    block = keep_ref[...] + other_ref[...]
    merged_ref[...] = block
    logs, out = terms(block, in_total_ref[chunk : chunk + 1, : block.shape[1]], new)
    if len(refs) > 2:
        logs, out = logs + refs[1][...], out + refs[2][...]
    row = lax.broadcasted_iota(I32, part_ref.shape, 0)
    logs = jnp.sum(logs.T, axis=0, keepdims=True)
    out = jnp.sum(out.T, axis=0, keepdims=True)
    total = jnp.sum(jnp.sum(in_total_ref[...], axis=0, keepdims=True), axis=1, keepdims=True)
    part_ref[...] = jnp.where(row == 0, logs, jnp.where(row == 1, out, total))


def finish_last(plan, new, in_total, keep, other, early):
    owned, width, total = keep.shape[0], plan[-1], sum(plan)
    at = (total - width) // width
    whole = pl.BlockSpec((owned, width), lambda k: (0, 0))
    lanes = [pl.BlockSpec((owned, 128), lambda k: (0, 0))] * 2
    return call(
        functools.partial(last_kernel, len(plan) - 1, new), 20 * owned * width, 12 * owned * width,
        grid=(1,),
        in_specs=[pl.BlockSpec(in_total.shape, lambda k: (0, 0)), whole, whole]
        + ([pl.BlockSpec(memory_space=pl.ANY)] + lanes if early else []),
        out_specs=[pl.BlockSpec((owned, width), lambda k: (0, at)), pl.BlockSpec((8, owned), lambda k: (0, 0))],
        out_shape=[jax.ShapeDtypeStruct((owned, total), F32), jax.ShapeDtypeStruct((8, owned), F32)],
        input_output_aliases={3: 0} if early else {},
    )(in_total, keep, other, *early)


def tags_of(ids, mine, capacity):
    rank = jnp.cumsum(mine.astype(I32), axis=1) - 1
    hit = mine[:, None, :] & (rank[:, None, :] == jnp.arange(capacity, dtype=I32)[None, :, None])
    return jnp.max(jnp.where(hit, ids[:, None, :], -1), axis=2)


def body(counts, merge_map):
    rows, cols = counts.shape
    groups, columns = lax.axis_size("blk"), lax.axis_size("col")
    blk, col = lax.axis_index("blk"), lax.axis_index("col")
    ids = merge_map[:, 0]
    new = ids.shape[0] // 2
    owned, owned_cols = new // groups, new // columns
    fanout = min(groups // 2, rows // 2)
    cap = rows // fanout
    half = groups // 2
    plan = widths(owned_cols)
    starts = [sum(plan[:q]) for q in range(len(plan))]
    row_labels = lax.dynamic_slice_in_dim(ids, blk * rows, rows, 0)
    col_labels = lax.dynamic_slice_in_dim(ids, col * cols, cols, 0)

    step_of = lax.rem(col_labels // owned_cols - col + columns, columns)
    col_pos = step_of * owned_cols + lax.rem(col_labels, owned_cols)
    mapped = (col_pos // owned).reshape(cols // rows, rows, 1) == jnp.arange(groups, dtype=I32)
    present = jnp.max(mapped.astype(I32), axis=1)

    owner = row_labels // owned
    table = (owner[:, None] == jnp.arange(groups, dtype=I32)[None, :]).astype(I32)
    rank = jnp.sum(jnp.cumsum(table, axis=0) * table, axis=1) - 1
    place = lax.rem(owner, half) * 2 + (owner // half != blk // half).astype(I32)
    row_pos = (place * cap + rank)[None, :]

    base = (blk // half) * half
    peers = lax.dynamic_slice_in_dim(ids.reshape(groups, rows), base, half, 0)
    take_pos = []
    for agg in (blk, lax.rem(blk + half, groups)):
        tags = tags_of(peers, peers // owned == agg, cap).reshape(-1)
        take_pos.append(jnp.where(tags < 0, -1, tags - agg * owned))
    take_pos = jnp.stack(take_pos)

    n = len(plan)
    carrier = max(n - 2, 0)
    keeps, others, halves, arrived = [], [], counts, []
    for q, width in enumerate(plan):
        parts = list(merge_columns(halves, col_pos[None, :], present, owned, columns, starts[q], width, q == 0))
        if q == 0:
            halves = parts.pop(0)
        for step in range(1, columns):
            parts[step] = lax.ppermute(parts[step], "col", [(i, (i + step) % columns) for i in range(columns)])
        arrived.append(parts)
    slotted, sums = [None] * n, [jnp.zeros((1, plan[carrier]), F32)] * 8
    for q in [i for i in range(n) if i != carrier]:
        slotted[q], column_sum = fill_slots(row_pos, arrived[q], half, groups * cap)
        sums[q] = jnp.pad(column_sum, ((0, 0), (0, plan[carrier] - plan[q])))
    known = jnp.concatenate(sums, axis=0)
    slotted[carrier], _ = fill_slots(row_pos, arrived[carrier], half, groups * cap, carrier, known)
    for q in range(n):
        got = lax.all_to_all(
            slotted[q], "blk", split_axis=0, concat_axis=0, tiled=True,
            axis_index_groups=[list(range(half)), list(range(half, groups))],
        )
        keep, send, *half_sums = merge_rows(take_pos, got, owned, q == carrier)
        others.append(lax.ppermute(send, "blk", [(i, (i + half) % groups) for i in range(groups)]))
        keeps.append(keep)
        if half_sums:
            in_total = half_sums[0] + others[q][owned:]
    chunks = list(zip(keeps, others))
    for q in range(max(min(2, n - 3), 0)):
        chunks[q] = (keeps[q] + others[q],)
    early = ()
    if n > 1:
        early = finish_early(plan, new, in_total, chunks[:-1])
    merged, part = finish_last(plan, new, in_total, keeps[-1], others[-1], early)
    if columns == 2:
        part += lax.ppermute(part, "col", [(0, 1), (1, 0)])
    else:
        part = lax.psum(part, "col")
    block_terms = part[0] / part[1] + jnp.log(part[2] / (part[1] * new))
    return (merged, block_terms)


def solution(mesh):
    placed = (P("blk", "col"), P())
    return jax.shard_map(body, mesh=mesh, in_specs=placed, out_specs=(P("blk", "col"), P("blk")), check_vma=False)
```

```python
import functools

import jax
import jax.numpy as jnp
from jax import lax
from jax.experimental import pallas as pl
from jax.experimental.pallas import tpu as pltpu
from jax.sharding import PartitionSpec as P

PARTS = (2, 4, 4, 4, 2)
VMEM = 24 * 2**20
F32, BF16, I32 = jnp.float32, jnp.bfloat16, jnp.int32


def widths(owned_cols):
    unit = owned_cols // sum(PARTS)
    return [p * unit for p in PARTS] if unit % 128 == 0 else [owned_cols]


def split(x):
    hi = x.astype(BF16)
    return hi, (x - hi.astype(F32)).astype(BF16)


def hot(labels, count, base=0):
    index = lax.broadcasted_iota(I32, (count, labels.shape[1]), 0) + base
    return jnp.where(index == labels, 1.0, 0.0).astype(BF16)


def mxu(a, b, dims):
    return lax.dot_general(a, b, (dims, ((), ())), preferred_element_type=F32)


def call(kernel, flops, nbytes, **kw):
    return pl.pallas_call(
        kernel,
        cost_estimate=pl.CostEstimate(flops=flops, bytes_accessed=nbytes, transcendentals=0),
        compiler_params=pltpu.CompilerParams(vmem_limit_bytes=VMEM),
        **kw,
    )


def columns_kernel(start, owned, first, targets, columns, present_ref, pos_ref, x_ref, *refs):
    sources = present_ref.shape[0]
    tile = x_ref.shape[1] // sources
    halves_ref, out_refs = (refs[0], refs[1:]) if first else (x_ref, refs)
    rows, width = out_refs[0].shape
    per_column = present_ref.shape[1] // columns
    for out_ref in out_refs:
        out_ref[...] = jnp.zeros_like(out_ref)

    def step(k, carry):
        at = pl.ds(pl.multiple_of(k * tile, tile), tile)
        if first:
            halves_ref[:rows, at], halves_ref[rows:, at] = split(x_ref[:, at])
        for c, out_ref in zip(targets, out_refs):
            for b in range(width // owned):
                block = c * per_column + start // owned + b

                @pl.when(present_ref[k, block] > 0)
                def _():
                    part = mxu(halves_ref[:, at], hot(pos_ref[:, at], owned, block * owned), ((1,), (1,)))
                    out_ref[:, b * owned : (b + 1) * owned] += part[:rows] + part[rows:]

        return carry

    lax.fori_loop(0, sources, step, 0)


def merge_columns(x, pos, present, owned, columns, start, width, first, targets):
    rows, cols = x.shape if first else (x.shape[0] // 2, x.shape[1])
    vmem = pl.BlockSpec(memory_space=pltpu.VMEM)
    halves = [jax.ShapeDtypeStruct((2 * rows, cols), BF16)] if first else []
    return call(
        functools.partial(columns_kernel, start, owned, first, targets, columns),
        2 * rows * cols * len(targets) * width, 4 * rows * (cols + len(targets) * width),
        in_specs=[pl.BlockSpec(memory_space=pltpu.SMEM), vmem, vmem],
        out_specs=[vmem] * (len(halves) + len(targets)),
        out_shape=halves + [jax.ShapeDtypeStruct((rows, width), F32)] * len(targets),
    )(present, pos, x)


def slots_kernel(carrier, pos_ref, *refs):
    ins, out_ref, sum_ref, table = refs[:-3], refs[-3], refs[-2], refs[-1]
    known_ref, ins = (ins[0], ins[1:]) if carrier is not None else (None, ins)
    peers, depth, tile = out_ref.shape
    used = table.shape[0] // peers

    @pl.when(pl.program_id(0) == 0)
    def _():
        table[...] = hot(pos_ref[...], table.shape[0])

    total = ins[0][...]
    for ref in ins[1:]:
        total += ref[...]
    column_sum = jnp.sum(total, axis=0, keepdims=True)
    sum_ref[...] = column_sum
    hi, lo = split(total)
    filled = mxu(table[...], hi, ((1,), (0,))) + mxu(table[...], lo, ((1,), (0,)))
    out_ref[:, :used] = filled.reshape(peers, used, tile)
    if carrier is not None:
        row = lax.broadcasted_iota(I32, known_ref.shape, 0)
        sums = jnp.where(row == carrier, column_sum, known_ref[...])
        out_ref[:, used:] = jnp.broadcast_to(sums[None], (peers, depth - used, tile))


def fill_slots(pos, ins, peers, slots, carrier=None, known=None):
    rows, width = ins[0].shape
    tile = min(width, 256)
    depth = slots // peers + (0 if carrier is None else 8)
    extra = [] if carrier is None else [known]
    return call(
        functools.partial(slots_kernel, carrier),
        4 * slots * rows * width, 4 * width * (rows * len(ins) + slots),
        grid=(width // tile,),
        in_specs=[pl.BlockSpec((1, rows), lambda k: (0, 0))]
        + [pl.BlockSpec((8, tile), lambda k: (0, k))] * len(extra)
        + [pl.BlockSpec((rows, tile), lambda k: (0, k))] * len(ins),
        out_specs=[pl.BlockSpec((peers, depth, tile), lambda k: (0, 0, k)), pl.BlockSpec((1, tile), lambda k: (0, k))],
        out_shape=[jax.ShapeDtypeStruct((peers, depth, width), F32), jax.ShapeDtypeStruct((1, width), F32)],
        scratch_shapes=[pltpu.VMEM((slots, rows), BF16)],
    )(pos, *extra, *ins)


def rows_kernel(owned, pos_ref, got_ref, out_ref):
    peers, depth, tile = got_ref.shape
    cap = pos_ref.shape[1] // peers
    for side in range(2):
        hi, lo = split(got_ref[:, side * cap : (side + 1) * cap].reshape(peers * cap, tile))
        table = hot(pos_ref[side : side + 1, :], owned)
        out_ref[side * owned : (side + 1) * owned] = mxu(table, hi, ((1,), (0,))) + mxu(table, lo, ((1,), (0,)))
    if depth > 2 * cap:
        out_ref[2 * owned :] = jnp.sum(got_ref[:, 2 * cap :], axis=0)


def merge_rows(pos, got, owned):
    peers, depth, width = got.shape
    slots = pos.shape[1]
    height = 2 * owned + depth - 2 * slots // peers
    tile = min(width, 256)
    return call(
        functools.partial(rows_kernel, owned), 8 * owned * slots * width, 4 * width * (2 * owned + 2 * slots),
        grid=(width // tile,),
        in_specs=[pl.BlockSpec((2, slots), lambda k: (0, 0)), pl.BlockSpec((peers, depth, tile), lambda k: (0, 0, k))],
        out_specs=pl.BlockSpec((height, tile), lambda k: (0, k)),
        out_shape=jax.ShapeDtypeStruct((height, width), F32),
    )(pos, got)


def fold(x):
    return sum(x[:, j : j + 128] for j in range(0, x.shape[1], 128))


def terms(block, in_total, new):
    return fold(block * jnp.log(block * (new / in_total))), fold(block)


def early_kernel(plan, new, in_total_ref, *refs):
    ins, (merged_ref, logs_ref, out_ref) = list(refs[:-3]), refs[-3:]
    start, logs, out = 0, 0.0, 0.0
    for q, (width, parts) in enumerate(plan):
        block = sum(ins.pop(0)[...] for _ in range(parts))
        merged_ref[:, start : start + width] = block
        more = terms(block, in_total_ref[q : q + 1, :width], new)
        logs, out, start = logs + more[0], out + more[1], start + width
    logs_ref[...], out_ref[...] = logs, out


def finish_early(plan, new, in_total, chunks):
    owned, total, done = chunks[0][0].shape[0], sum(plan), sum(plan[:-1])
    tile = min(owned, 64)
    lanes = pl.BlockSpec((tile, 128), lambda k: (k, 0))
    return call(
        functools.partial(early_kernel, [(w, len(c)) for w, c in zip(plan, chunks)], new),
        20 * owned * done, 12 * owned * done,
        grid=(owned // tile,),
        in_specs=[pl.BlockSpec(in_total.shape, lambda k: (0, 0))]
        + [pl.BlockSpec((tile, w), lambda k: (k, 0)) for w, c in zip(plan, chunks) for _ in c],
        out_specs=[pl.BlockSpec((tile, done), lambda k: (k, 0)), lanes, lanes],
        out_shape=[jax.ShapeDtypeStruct((owned, total), F32)] + [jax.ShapeDtypeStruct((owned, 128), F32)] * 2,
    )(in_total, *(x for c in chunks for x in c))


def last_kernel(chunk, new, in_total_ref, keep_ref, other_ref, *refs):
    merged_ref, part_ref = refs[-2:]
    block = keep_ref[...] + other_ref[...]
    merged_ref[...] = block
    logs, out = terms(block, in_total_ref[chunk : chunk + 1, : block.shape[1]], new)
    if len(refs) > 2:
        logs, out = logs + refs[1][...], out + refs[2][...]
    row = lax.broadcasted_iota(I32, part_ref.shape, 0)
    logs = jnp.sum(logs.T, axis=0, keepdims=True)
    out = jnp.sum(out.T, axis=0, keepdims=True)
    total = jnp.sum(jnp.sum(in_total_ref[...], axis=0, keepdims=True), axis=1, keepdims=True)
    part_ref[...] = jnp.where(row == 0, logs, jnp.where(row == 1, out, total))


def finish_last(plan, new, in_total, keep, other, early):
    owned, width, total = keep.shape[0], plan[-1], sum(plan)
    at = (total - width) // width
    whole = pl.BlockSpec((owned, width), lambda k: (0, 0))
    lanes = [pl.BlockSpec((owned, 128), lambda k: (0, 0))] * 2
    return call(
        functools.partial(last_kernel, len(plan) - 1, new), 20 * owned * width, 12 * owned * width,
        grid=(1,),
        in_specs=[pl.BlockSpec(in_total.shape, lambda k: (0, 0)), whole, whole]
        + ([pl.BlockSpec(memory_space=pl.ANY)] + lanes if early else []),
        out_specs=[pl.BlockSpec((owned, width), lambda k: (0, at)), pl.BlockSpec((8, owned), lambda k: (0, 0))],
        out_shape=[jax.ShapeDtypeStruct((owned, total), F32), jax.ShapeDtypeStruct((8, owned), F32)],
        input_output_aliases={3: 0} if early else {},
    )(in_total, keep, other, *early)


def tags_of(ids, mine, capacity):
    rank = jnp.cumsum(mine.astype(I32), axis=1) - 1
    hit = mine[:, None, :] & (rank[:, None, :] == jnp.arange(capacity, dtype=I32)[None, :, None])
    return jnp.max(jnp.where(hit, ids[:, None, :], -1), axis=2)


def body(counts, merge_map):
    rows, cols = counts.shape
    groups, columns = lax.axis_size("blk"), lax.axis_size("col")
    blk, col = lax.axis_index("blk"), lax.axis_index("col")
    ids = merge_map[:, 0]
    new = ids.shape[0] // 2
    owned, owned_cols = new // groups, new // columns
    fanout = min(groups // 2, rows // 2)
    cap = rows // fanout
    half = groups // 2
    plan = widths(owned_cols)
    starts = [sum(plan[:q]) for q in range(len(plan))]
    row_labels = lax.dynamic_slice_in_dim(ids, blk * rows, rows, 0)
    col_labels = lax.dynamic_slice_in_dim(ids, col * cols, cols, 0)

    step_of = lax.rem(col_labels // owned_cols - col + columns, columns)
    col_pos = step_of * owned_cols + lax.rem(col_labels, owned_cols)
    mapped = (col_pos // owned).reshape(cols // rows, rows, 1) == jnp.arange(groups, dtype=I32)
    present = jnp.max(mapped.astype(I32), axis=1)

    owner = row_labels // owned
    table = (owner[:, None] == jnp.arange(groups, dtype=I32)[None, :]).astype(I32)
    rank = jnp.sum(jnp.cumsum(table, axis=0) * table, axis=1) - 1
    side_of = blk // half
    within = lax.rem(owner, half)
    quarter = half // 2
    inner = owner // half != side_of
    aggregator = jnp.where(inner, 1 - side_of, side_of) * quarter + lax.rem(within, quarter)
    place = aggregator * 2 + (within // quarter == side_of).astype(I32)
    row_pos = (place * cap + rank)[None, :]

    base = (blk // half) * half
    peers = lax.dynamic_slice_in_dim(ids.reshape(groups, rows), base, half, 0)
    take_pos = []
    outer = lax.rem(blk, half) // quarter == side_of
    served = jnp.where(outer, side_of, 1 - side_of) * half + lax.rem(blk, quarter)
    for agg in (served + (1 - side_of) * quarter, served + side_of * quarter):
        tags = tags_of(peers, peers // owned == agg, cap).reshape(-1)
        take_pos.append(jnp.where(tags < 0, -1, tags - agg * owned))
    take_pos = jnp.stack(take_pos)

    n = len(plan)
    carrier = max(n - 2, 0)
    keeps, others, halves, arrived = [], [], None, []
    for q, width in enumerate(plan):
        merge = functools.partial(merge_columns, pos=col_pos[None, :], present=present, owned=owned, columns=columns)
        if q:
            parts = merge(halves, start=starts[q], width=width, first=False, targets=tuple(range(columns)))
        else:
            halves, *parts = merge(counts, start=0, width=width, first=True, targets=tuple(range(1, columns)))
        if q == 0:
            parts = [*merge(halves, start=0, width=width, first=False, targets=(0,)), *parts]
        parts = list(parts)
        for step in range(1, columns):
            parts[step] = lax.ppermute(parts[step], "col", [(i, (i + step) % columns) for i in range(columns)])
        arrived.append(parts)
    slotted, sums = [None] * n, [jnp.zeros((1, plan[carrier]), F32)] * 8
    for q in [i for i in range(n) if i != carrier]:
        slotted[q], column_sum = fill_slots(row_pos, arrived[q], half, groups * cap)
        sums[q] = jnp.pad(column_sum, ((0, 0), (0, plan[carrier] - plan[q])))
    known = jnp.concatenate(sums, axis=0)
    slotted[carrier], _ = fill_slots(row_pos, arrived[carrier], half, groups * cap, carrier, known)
    for q in range(n):
        got = lax.all_to_all(
            slotted[q], "blk", split_axis=0, concat_axis=0, tiled=True,
            axis_index_groups=[list(range(half)), list(range(half, groups))],
        )
        both = merge_rows(take_pos, got, owned)
        middle = [(quarter + r, half + r) for r in range(quarter)]
        across = lax.ppermute(both, "blk", middle + [(j, i) for i, j in middle])
        mine = jnp.where(outer, both[:2 * owned], across[:2 * owned])
        send, keep = mine[:owned], mine[owned:]
        if q == carrier:
            send = jnp.concatenate([send, across[2 * owned :]], axis=0)
        pairs = [(h * half + r, h * half + quarter + r) for h in range(2) for r in range(quarter)]
        others.append(lax.ppermute(send, "blk", pairs + [(j, i) for i, j in pairs]))
        keeps.append(keep)
        if q == carrier:
            in_total = both[2 * owned :] + jnp.where(outer, others[q][owned:], across[2 * owned :])
    chunks = list(zip(keeps, others))
    for q in range(max(min(2, n - 3), 0)):
        chunks[q] = (keeps[q] + others[q],)
    early = ()
    if n > 1:
        early = finish_early(plan, new, in_total, chunks[:-1])
    merged, part = finish_last(plan, new, in_total, keeps[-1], others[-1], early)
    if columns == 2:
        part += lax.ppermute(part, "col", [(0, 1), (1, 0)])
    else:
        part = lax.psum(part, "col")
    block_terms = part[0] / part[1] + jnp.log(part[2] / (part[1] * new))
    return (merged, block_terms)


def solution(mesh):
    placed = (P("blk", "col"), P())
    return jax.shard_map(body, mesh=mesh, in_specs=placed, out_specs=(P("blk", "col"), P("blk")), check_vma=False)
```
